32 devices in a mesh: child: 4 (over z), rows: 8 (over y, x, core).
Axes of the slice: x: 2, y: 2, z: 4, core: 2. Of those that a mesh axis runs over, the one named last changes fastest.
Arguments:
- omega: bfloat16 [4, 8192, 512], P('child', 'rows'), may hold values from -6 to 6
- leaf_diag: bfloat16 [4, 32, 256, 256], P('child', 'rows'), may hold values from -0.375 to 0.375
- leaf_u: bfloat16 [4, 8192, 128], P('child', 'rows'), may hold values from -0.5 to 0.5
- leaf_v: bfloat16 [4, 8192, 128], P('child', 'rows'), may hold values from -0.375 to 0.375
- coupling: bfloat16 [4, 4096, 4096], P('child', 'rows'), may hold values from -0.09375 to 0.09375
- child_map: int32 [4, 64], P('child', 'rows'), may hold values from 0 to 95, as said below
Outputs:
- parent_rows: float32 [3, 4096, 512], P(None, ('child', 'rows'))
The draws below stay inside these ranges and needn't reach their ends.
Inputs may be any that keep to these rules, and one draw needn't show every extreme that they name: `child_map`: child block b of every child maps to one of the parent blocks 3 * (b // 2), 3 * (b // 2) + 1, 3 * (b // 2) + 2, and blocks 2 k and 2 k + 1 map to two different ones of their triple, the lower first.
All inputs are finite; a program needn't handle non-finite values.
Results may differ from the reference program's by a relative error of at most 0.004.
Values may be sent and summed in bfloat16 or wider, within the bound.
A program may use at most 128 MiB of HBM per device.

```python
import jax
import jax.numpy as jnp
from jax import lax

L = 256
R = 128
S = 512
LEAF_DEV = 4
NLEAF = 32
NC = 8192
NCB = 64
PBLK_DEV = 3
N_CHILD = 4
N_ROWS = 8


def draw_child_map(key, part):
    pairs = NCB // 2
    omitted = jax.random.randint(key, (N_CHILD, pairs), 0, 3)
    first = jnp.where(omitted == 0, 1, 0)
    second = jnp.where(omitted == 2, 1, 2)
    triple = 3 * jnp.arange(pairs, dtype=jnp.int32)[None, :]
    both = jnp.stack([triple + first, triple + second], axis=2)
    return both.reshape(N_CHILD, NCB).astype(jnp.int32)


def levels(stream_key, dims, split, least, largest):
    def one(position, shards_of):
        steps = jax.random.uniform(jax.random.fold_in(jax.random.fold_in(stream_key, 6), position), (shards_of,), jnp.float32, least / len(split), largest / len(split))
        return jnp.repeat(jnp.exp(steps), dims[position] // shards_of).reshape((-1,) + (1,) * (len(dims) - position - 1))

    gain = one(*split[0])
    for cut in split[1:]:
        gain = gain * one(*cut)
    return gain


def bell_draw(key, extent, scale, reach, pieces=(), kind=jnp.bfloat16):
    result = scale * jax.random.normal(key, extent, jnp.float32)
    if pieces:
        result = result * levels(key, extent, pieces, -0.22, 0.18)
    return jnp.clip(result, -reach, reach).astype(kind)


def setup_inputs(seed: int = 0) -> dict:
    seeds = jax.random.split(jax.random.key(seed), 7)
    return {
        "omega": bell_draw(seeds[0], (N_CHILD, NC, S), 1.0, 6.0, ((0, 4), (1, 8))),
        "leaf_diag": bell_draw(seeds[1], (N_CHILD, NLEAF, L, L), L ** -0.5, 0.375, ((0, 4), (1, 8))),
        "leaf_u": bell_draw(seeds[2], (N_CHILD, NC, R), R ** -0.5, 0.5, ((0, 4), (1, 8))),
        "leaf_v": bell_draw(seeds[3], (N_CHILD, NC, R), L ** -0.5, 0.375, ((0, 4), (1, 8))),
        "coupling": bell_draw(seeds[4], (N_CHILD, NLEAF * R, NLEAF * R), (NLEAF * R) ** -0.5, 0.09375, ((0, 4), (1, 8))),
        "child_map": draw_child_map(jax.random.fold_in(seeds[6], 71), 0),
    }


def reference(omega, leaf_diag, leaf_u, leaf_v, coupling, child_map):
    block_rows = L // 2
    parent_count = 3 * LEAF_DEV * N_ROWS
    parent = jnp.zeros((parent_count, block_rows, S), jnp.float32)
    for child_index in range(N_CHILD):
        omega_leaves = omega[child_index].astype(jnp.float32).reshape(NLEAF, L, S)
        basis_in = leaf_v[child_index].astype(jnp.float32).reshape(NLEAF, L, R)
        basis_out = leaf_u[child_index].astype(jnp.float32).reshape(NLEAF, L, R)
        sampled = jnp.einsum("nlr,nls->nrs", basis_in, omega_leaves).astype(jnp.bfloat16).reshape(NLEAF * R, S)
        coupled = jnp.dot(coupling[child_index], sampled, preferred_element_type=jnp.float32).astype(jnp.bfloat16)
        coupled = lax.optimization_barrier(coupled).astype(jnp.float32).reshape(NLEAF, R, S)
        local_part = jnp.einsum("nij,njs->nis", leaf_diag[child_index].astype(jnp.float32), omega_leaves)
        local_part = local_part + jnp.einsum("nlr,nrs->nls", basis_out, coupled)
        update = lax.optimization_barrier(local_part.astype(jnp.bfloat16)).astype(jnp.float32)
        update = update.reshape(2 * NLEAF, block_rows, S)
        parent = parent.at[child_map[child_index].astype(jnp.int32)].add(update)
    parent = parent.reshape(N_ROWS, N_CHILD, PBLK_DEV, block_rows, S)
    parent = jnp.transpose(parent, (2, 1, 0, 3, 4))
    return parent.reshape(PBLK_DEV, N_CHILD * N_ROWS * block_rows, S)
```

```python
import functools

import jax
import jax.numpy as jnp
from jax import lax
from jax.experimental import pallas as pl
from jax.experimental.pallas import tpu as pltpu
from jax.sharding import PartitionSpec as P

MESH = pl.DeviceIdType.MESH
WIDTH = 128
HALF = WIDTH // 2


def dot(a, b):
    return jnp.dot(a, b, preferred_element_type=jnp.float32)


def left_lanes(rows):
    return lax.broadcasted_iota(jnp.int32, (rows, WIDTH), 1) < HALF


def kernel(
    n_child, n_rows, omega_hbm, v_hbm, map_hbm, diag_hbm, u_hbm, coupling_hbm, out,
    omega, v, diag, u, coupling, gathered, local_part, total, coupled,
    halves, update, sums, halves_in, inner_in, near_in, far_in, maps, slots, slots_in, inner_slots,
    load_sem, ici_send, ici_recv, fwd_send, fwd_recv, core_send, core_recv,
    half_send, half_recv, inner_send, inner_recv, near_send, near_recv, far_send, far_recv,
    map_send, map_recv,
):
    groups, depth = gathered.shape[0], gathered.shape[1]
    leaves, leaf = diag.shape[0], diag.shape[1]
    rank = u.shape[1]
    block = leaves * rank
    chips = n_rows // 2
    last = groups
    c = lax.axis_index("child")
    r = lax.axis_index("rows")
    chip, core = r // 2, r % 2
    partner = chip * 2 + 1 - core

    forward = chips == 4
    if forward:
        x, y = chip % 2, chip // 2
        x_near = (y * 2 + 1 - x) * 2
        y_near = ((1 - y) * 2 + x) * 2
        first = x_near * (1 - core) + y_near * core
        second = y_near * (1 - core) + x_near * core
        across = ((1 - y) * 2 + 1 - x) * 2
        direct = [(second + core, second + core), (first + core, first + core)]
        other = [first + 1 - core, second + 1 - core]
    else:
        direct = [
            (((chip + d) % chips) * 2 + core, ((chip + chips - d) % chips) * 2 + core)
            for d in range(1, chips)
        ]
        other = [((chip + chips - d) % chips) * 2 + 1 - core for d in range(1, chips)]
    sources = [r] + [s for _, s in direct]
    other = [partner] + other
    if forward:
        sources.append(across + core)
        other.append(across + 1 - core)

    high = c // 2
    beside = c + 1 - 2 * (c % 2)
    peers = [3 - c, (c + 2) % 4, beside]
    is_inner = (c == 1) | (c == 2)
    is_outer = (c == 0) | (c == 3)
    ends = [3 - 3 * high, 2 - high]

    barrier = pltpu.get_barrier_semaphore()
    for to, _ in direct + [(partner, partner)]:
        pl.semaphore_signal(barrier, inc=1, device_id=(c, to), device_id_type=MESH)
    for to in peers:
        pl.semaphore_signal(barrier, inc=1, device_id=(to, r), device_id_type=MESH)

    loads = [
        pltpu.make_async_copy(v_hbm.at[0], v, load_sem.at[0]),
        pltpu.make_async_copy(
            omega_hbm.at[0, :, :WIDTH], omega.at[:, :WIDTH], load_sem.at[1]
        ),
        pltpu.make_async_copy(
            omega_hbm.at[0, :, WIDTH:], omega.at[:, WIDTH:], load_sem.at[2]
        ),
        pltpu.make_async_copy(map_hbm, maps, load_sem.at[3]),
        pltpu.make_async_copy(diag_hbm.at[0], diag, load_sem.at[4]),
        pltpu.make_async_copy(coupling_hbm.at[0], coupling, load_sem.at[5]),
        pltpu.make_async_copy(u_hbm.at[0], u, load_sem.at[6]),
    ]
    for load in loads:
        load.start()

    def packed(s):
        return s in (0, last)

    def piece(s, source):
        if packed(s):
            base = 0 if s == 0 else depth // 2
            size = block // 2
            return 0, pl.ds(pl.multiple_of(base + source * size, size), size)
        return s, pl.ds(pl.multiple_of(source * block, block), block)

    def rows_of(s, source):
        return gathered.at[piece(s, source)]

    def columns(g):
        return slice(g * WIDTH, (g + 1) * WIDTH)

    def project(i, cols):
        rows = slice(i * leaf, (i + 1) * leaf)
        return lax.dot_general(
            v[rows, :], omega[rows, cols], (((0,), (0,)), ((), ())),
            preferred_element_type=jnp.float32,
        )

    def project_first():
        mask = left_lanes(rank)
        for i in range(leaves // 2):
            low = project(i, columns(0))
            up = pltpu.roll(project(i + leaves // 2, columns(0)), HALF, 1)
            size = block // 2
            at = pl.multiple_of(r * size + i * rank, rank)
            gathered[0, pl.ds(at, rank), :] = jnp.where(mask, low, up).astype(jnp.bfloat16)
            at = pl.multiple_of(depth // 2 + r * size + i * rank, rank)
            gathered[0, pl.ds(at, rank), :] = jnp.where(mask, up, low).astype(jnp.bfloat16)

    def project_rest():
        for i in range(leaves):
            projected = project(i, slice(WIDTH, groups * WIDTH)).astype(jnp.bfloat16)
            at = pl.ds(pl.multiple_of(r * block + i * rank, rank), rank)
            for g in range(1, groups):
                gathered[g, at, :] = projected[:, (g - 1) * WIDTH : g * WIDTH]

    def remote(src, dst, send, recv, to):
        return pltpu.make_async_remote_copy(
            src_ref=src, dst_ref=dst, send_sem=send, recv_sem=recv,
            device_id=to, device_id_type=MESH,
        )

    def ici(t, s):
        at = rows_of(s, r)
        return remote(at, at, ici_send.at[t, s], ici_recv.at[t, s], (c, direct[t][0]))

    def ici_in(t, s):
        at = rows_of(s, direct[t][1])
        return remote(at, at, ici_send.at[t, s], ici_recv.at[t, s], (c, direct[t][0]))

    def fwd(s):
        at = rows_of(s, direct[0][1])
        return remote(at, at, fwd_send.at[s], fwd_recv.at[s], (c, direct[1][0]))

    def fwd_in(s):
        at = rows_of(s, sources[-1])
        return remote(at, at, fwd_send.at[s], fwd_recv.at[s], (c, direct[1][0]))

    def across_core(t, s, who):
        at = rows_of(s, who[t])
        return remote(at, at, core_send.at[t, s], core_recv.at[t, s], (c, partner))

    def half_to(j, h):
        return remote(
            halves.at[h, peers[j]], halves_in.at[h, j],
            half_send.at[h, j], half_recv.at[h, j], (peers[j], r),
        )

    def to_inner(e, g):
        return remote(
            update.at[g - 1, e], inner_in.at[g - 1, e],
            inner_send.at[g - 1, e], inner_recv.at[g - 1, e], (beside, r),
        )

    def to_near(g):
        return remote(
            update.at[g - 1, 2], near_in.at[g - 1],
            near_send.at[g - 1], near_recv.at[g - 1], (beside, r),
        )

    def to_far(e, g):
        return remote(
            sums.at[g - 1, e], far_in.at[g - 1],
            far_send.at[g - 1, e], far_recv.at[g - 1], (ends[e], r),
        )

    def map_to_peer(j):
        return remote(
            slots.at[peers[j]], slots_in.at[j], map_send.at[j], map_recv.at[j], (peers[j], r)
        )

    def map_to_inner(e):
        return remote(
            slots.at[ends[e]], inner_slots.at[e],
            map_send.at[3 + e], map_recv.at[3 + e], (beside, r),
        )

    sent = []

    def start(copy):
        copy.start()
        sent.append(copy)

    def send_own(t, s):
        if s <= last:
            start(ici(t, s))

    def send_core(s):
        if s <= last:
            start(across_core(0, s, sources))

    def arrive(t, s):
        if s <= last:
            ici_in(t, s).wait_recv()
            if forward and t == 0:
                start(fwd(s))
            start(across_core(t + 1, s, sources))

    def arrive_across(s):
        fwd_in(s).wait_recv()
        start(across_core(len(sources) - 1, s, sources))

    def part(s, source, fresh=False):
        k = s % 2
        if packed(s):
            g, at = piece(s, source)
            value = gathered[g, at, :]
            size = block // 2
            for h in range(2):
                cols = pl.ds(pl.multiple_of(source * block + h * size, size), size)
                term = dot(coupling[:, cols], value)
                total[k, h] = term if fresh else total[k, h] + term
        else:
            g, at = piece(s, source)
            term = dot(coupling[:, at], gathered[g, at, :])
            total[k, 0] = term if fresh else total[k, 0] + term

    def from_core(t, s):
        across_core(t, s, other).wait_recv()
        part(s, other[t])

    def settle(s):
        k = s % 2
        if packed(s):
            mask = left_lanes(block)
            a, b = (0, 1) if s == 0 else (1, 0)
            mixed = jnp.where(mask, total[k, a], total[k, b])
            coupled[k] = (mixed + pltpu.roll(mixed, HALF, 1)).astype(jnp.bfloat16)
        else:
            coupled[k] = total[k, 0].astype(jnp.bfloat16)

    def product(s, i):
        rows = pl.ds(pl.multiple_of(i * leaf, leaf), leaf)
        return dot(u[rows, :], coupled[s % 2, pl.ds(pl.multiple_of(i * rank, rank), rank), :])

    def local_rows(i):
        for g in range(groups):
            rows = slice(i * leaf, (i + 1) * leaf)
            value = dot(diag[i], omega[rows, columns(g)])
            if g == 0:
                mask = left_lanes(leaf // 2)
                low, up = value[: leaf // 2], pltpu.roll(value[leaf // 2 :], HALF, 1)
                local_part[i * leaf : i * leaf + leaf // 2, :WIDTH] = jnp.where(mask, low, up)
                local_part[i * leaf + leaf // 2 : (i + 1) * leaf, :WIDTH] = jnp.where(mask, up, low)
            else:
                local_part[rows, columns(g)] = value

    def finish_half(s):
        h = 0 if s == 0 else 1
        mask = left_lanes(leaf // 2)
        for j, i in enumerate(peers + [c]):
            value = product(s, i)
            low, up = value[: leaf // 2], value[leaf // 2 :]
            mixed = jnp.where(mask, low, up) if h == 0 else jnp.where(mask, up, low)
            rows = pl.ds(pl.multiple_of(i * leaf + h * (leaf // 2), leaf // 2), leaf // 2)
            halves[h, i] = (mixed + local_part[rows, :WIDTH]).astype(jnp.bfloat16)
            if j < len(peers):
                start(half_to(j, h))

    def finish_group(g):
        for e, i in enumerate(ends + [beside, c]):
            rows = pl.ds(pl.multiple_of(i * leaf, leaf), leaf)
            value = product(g, i) + local_part[rows, columns(g)]
            update[g - 1, e] = value.astype(jnp.bfloat16)
            if e < 2:
                @pl.when(is_outer)
                def _():
                    to_inner(e, g).start()
            elif e == 2:
                start(to_near(g))

    def finish(s):
        settle(s)
        if packed(s):
            finish_half(s)
        else:
            finish_group(s)

    def spread(low, up, slot, q):
        s0, s1 = slot[0:1, :], slot[4:5, :]
        return jnp.where(s0 == float(q), low, jnp.where(s1 == float(q), up, 0.0))

    def combine(g):
        if 1 <= g < last:
            @pl.when(is_inner)
            def _():
                for e in range(2):
                    to_inner(e, g).wait_recv()
                    own = update[g - 1, e].astype(jnp.float32)
                    got = inner_in[g - 1, e].astype(jnp.float32)
                    own_slot, got_slot = slots[ends[e]], inner_slots[e]
                    for q in range(3):
                        value = spread(
                            own[: leaf // 2], own[leaf // 2 :], own_slot, q
                        ) + spread(got[: leaf // 2], got[leaf // 2 :], got_slot, q)
                        sums[g - 1, e, q * (leaf // 2) : (q + 1) * (leaf // 2), :] = value.astype(
                            jnp.bfloat16
                        )
                    to_far(e, g).start()

    def final(g):
        if 1 <= g < last:
            to_near(g).wait_recv()
            to_far(0, g).wait_recv()
            own = update[g - 1, 3].astype(jnp.float32)
            got = near_in[g - 1].astype(jnp.float32)
            own_slot, got_slot = slots[c], slots_in[2]
            for q in range(3):
                far = far_in[g - 1, q * (leaf // 2) : (q + 1) * (leaf // 2), :]
                out[q, :, columns(g)] = (
                    spread(own[: leaf // 2], own[leaf // 2 :], own_slot, q)
                    + spread(got[: leaf // 2], got[leaf // 2 :], got_slot, q)
                    + far.astype(jnp.float32)
                )

    def final_halves():
        mask = left_lanes(leaf // 2)
        for j in [3, 2, 1, 0]:
            if j == 3:
                a, b, slot = halves[0, c], halves[1, c], slots[c]
            else:
                half_to(j, 1).wait_recv()
                a, b, slot = halves_in[0, j], halves_in[1, j], slots_in[j]
            a, b = a.astype(jnp.float32), b.astype(jnp.float32)
            low = jnp.where(mask, a, b)
            up = pltpu.roll(jnp.where(mask, b, a), HALF, 1)
            for q in range(3):
                term = spread(low, up, slot, q)
                out[q, :, :WIDTH] = term if j == 3 else out[q, :, :WIDTH] + term

    loads[0].wait()
    loads[1].wait()
    project_first()
    pl.semaphore_wait(barrier, len(direct) + 1 + len(peers))
    for t in reversed(range(len(direct))):
        send_own(t, 0)
    send_core(0)
    loads[2].wait()
    project_rest()
    send_own(0, 1)
    if not forward:
        for t in range(1, len(direct)):
            send_own(t, 1)
        send_core(1)
    loads[3].wait()
    for i in range(leaves):
        for b in range(2):
            slot = maps[0, 2 * i + b] - 3 * (r * leaves + i)
            slots[i, 4 * b : 4 * b + 4, :] = jnp.full((4, WIDTH), slot, jnp.int32).astype(
                jnp.float32
            )
    for j in range(len(peers)):
        start(map_to_peer(j))

    @pl.when(is_outer)
    def _():
        for e in range(2):
            map_to_inner(e).start()

    loads[4].wait()
    for i in range(leaves):
        local_rows(i)
    loads[5].wait()
    loads[6].wait()

    if forward:
        arrive(0, 0)
        send_own(1, 1)
        send_core(1)
        send_own(0, 2)
        arrive(1, 0)
        part(0, sources[0], True)
        part(0, sources[1])
        part(0, sources[2])
    for j in range(len(peers)):
        map_to_peer(j).wait_recv()

    @pl.when(is_inner)
    def _():
        for e in range(2):
            map_to_inner(e).wait_recv()

    for s in range(last + 1):
        if forward:
            arrive(0, s + 1)
            send_own(1, s + 2)
            send_core(s + 2)
            send_own(0, s + 3)
            from_core(0, s)
            arrive_across(s)
            from_core(1, s)
            from_core(2, s)
            part(s, sources[3])
            arrive(1, s + 1)
            if s < last:
                part(s + 1, sources[0], True)
                part(s + 1, sources[1])
            from_core(3, s)
            finish(s)
            if s < last:
                part(s + 1, sources[2])
        else:
            for t in range(len(direct)):
                arrive(t, s)
                send_own(t, s + 2)
            send_core(s + 2)
            for t in range(len(other)):
                across_core(t, s, other).wait_recv()
            part(s, 0, True)

            def more(i, carry, s=s):
                part(s, i)
                return carry

            lax.fori_loop(1, n_rows, more, 0)
            finish(s)
        combine(s - 1)
        final(s - 2)
    for g in range(max(1, last - 1), last):
        if g > last - 1:
            combine(g)
        final(g)
    for j in range(len(peers)):
        half_to(j, 0).wait_recv()
    final_halves()
    for copy in sent:
        copy.wait_send()

    @pl.when(is_outer)
    def _():
        for e in range(2):
            map_to_inner(e).wait_send()
            for g in range(1, last):
                to_inner(e, g).wait_send()

    @pl.when(is_inner)
    def _():
        for e in range(2):
            for g in range(1, last):
                to_far(e, g).wait_send()


def write(value, out, sem):
    copies = [
        pltpu.make_async_copy(value.at[q], out.at[q], sem.at[q]) for q in range(out.shape[0])
    ]
    for copy in copies:
        copy.start()
    for copy in copies:
        copy.wait()


def solution(mesh):
    n_child, n_rows = mesh.shape["child"], mesh.shape["rows"]

    def on_device(omega, leaf_diag, leaf_u, leaf_v, coupling, child_map):
        leaves, leaf = leaf_diag.shape[1], leaf_diag.shape[2]
        rank, samples = leaf_u.shape[2], omega.shape[2]
        groups = samples // WIDTH
        steps = groups + 1
        block, depth = coupling.shape[1], coupling.shape[2]
        chips = n_rows // 2
        direct = 2 if chips == 4 else chips - 1
        everyone = 1 + direct + (chips == 4)
        peers = n_child - 1
        vmem = pltpu.VMEM
        bf16, f32 = jnp.bfloat16, jnp.float32
        dma = pltpu.SemaphoreType.DMA
        anywhere = pl.BlockSpec(memory_space=pl.ANY)
        shape = (3, leaf // 2, samples)
        rest = groups - 1
        value = pl.pallas_call(
            functools.partial(kernel, n_child, n_rows),
            out_shape=vmem(shape, f32),
            in_specs=[anywhere] * 6,
            out_specs=pl.BlockSpec(memory_space=vmem),
            scratch_shapes=[
                vmem((leaves * leaf, samples), bf16),
                vmem((leaves * leaf, rank), bf16),
                vmem((leaves, leaf, leaf), bf16),
                vmem((leaves * leaf, rank), bf16),
                vmem((block, depth), bf16),
                vmem((groups, depth, WIDTH), bf16),
                vmem((leaves * leaf, samples), f32),
                vmem((2, 2, block, WIDTH), f32),
                vmem((2, block, WIDTH), bf16),
                vmem((2, leaves, leaf // 2, WIDTH), bf16),
                vmem((rest, 4, leaf, WIDTH), bf16),
                vmem((rest, 2, 3 * leaf // 2, WIDTH), bf16),
                vmem((2, peers, leaf // 2, WIDTH), bf16),
                vmem((rest, 2, leaf, WIDTH), bf16),
                vmem((rest, leaf, WIDTH), bf16),
                vmem((rest, 3 * leaf // 2, WIDTH), bf16),
                pltpu.SMEM(child_map.shape, jnp.int32),
                vmem((leaves, 8, WIDTH), f32),
                vmem((peers, 8, WIDTH), f32),
                vmem((2, 8, WIDTH), f32),
                dma((7,)),
                dma((direct, steps)),
                dma((direct, steps)),
                dma((steps,)),
                dma((steps,)),
                dma((everyone, steps)),
                dma((everyone, steps)),
                dma((2, peers)),
                dma((2, peers)),
                dma((rest, 2)),
                dma((rest, 2)),
                dma((rest,)),
                dma((rest,)),
                dma((rest, 2)),
                dma((rest,)),
                dma((peers + 2,)),
                dma((peers + 2,)),
            ],
            compiler_params=pltpu.CompilerParams(
                collective_id=0, has_side_effects=True, vmem_limit_bytes=52 * 1024 * 1024
            ),
        )(*[
            pltpu.with_memory_space_constraint(array, pltpu.HBM)
            for array in (omega, leaf_v, child_map, leaf_diag, leaf_u, coupling)
        ])
        value = pltpu.with_memory_space_constraint(value, vmem)
        return pl.pallas_call(
            write,
            out_shape=jax.ShapeDtypeStruct(shape, f32),
            in_specs=[pl.BlockSpec(memory_space=vmem)],
            out_specs=anywhere,
            scratch_shapes=[dma((3,))],
        )(value)

    placed = (
        P("child", "rows", None),
        P("child", "rows", None, None),
        P("child", "rows", None),
        P("child", "rows", None),
        P("child", "rows", None),
        P("child", "rows"),
    )
    return jax.shard_map(
        on_device,
        mesh=mesh,
        in_specs=placed,
        out_specs=P(None, ("child", "rows"), None),
        check_vma=False,
    )
```

```python
import functools

import jax
import jax.numpy as jnp
from jax import lax
from jax.experimental import pallas as pl
from jax.experimental.pallas import tpu as pltpu
from jax.sharding import PartitionSpec as P

MESH = pl.DeviceIdType.MESH
WIDTH = 128
HALF = WIDTH // 2
AHEAD = 2
LAG = 2
DONE = 6


def dot(a, b):
    return jnp.dot(a, b, preferred_element_type=jnp.float32)


def left_lanes(rows):
    return lax.broadcasted_iota(jnp.int32, (rows, WIDTH), 1) < HALF


def kernel(
    n_child, n_rows, omega_hbm, v_hbm, map_hbm, diag_hbm, u_hbm, coupling_hbm, out,
    omega, v, diag, u, coupling, gathered, mine, near_total, local_part, total, coupled,
    update, sums, peer_in, inner_in, far_in, halves, maps, slots, slots_in, inner_slots,
    load_sem, ici_send, ici_recv, fwd_send, fwd_recv, core_send, core_recv, mine_send, mine_recv,
    peer_send, near_recv, peer_recv, inner_send, inner_recv, far_send, far_recv,
    map_send, map_recv, ready,
):
    groups, depth = gathered.shape[0], gathered.shape[1]
    leaves, leaf = diag.shape[0], diag.shape[1]
    rank = u.shape[1]
    block = leaves * rank
    chips = n_rows // 2
    steps = 2 * groups
    last = steps - 1
    c = lax.axis_index("child")
    r = lax.axis_index("rows")
    chip, core = r // 2, r % 2
    partner = chip * 2 + 1 - core

    forward = chips == 4
    if forward:
        x, y = chip % 2, chip // 2
        x_near = (y * 2 + 1 - x) * 2
        y_near = ((1 - y) * 2 + x) * 2
        first = x_near * (1 - core) + y_near * core
        second = y_near * (1 - core) + x_near * core
        across = ((1 - y) * 2 + 1 - x) * 2
        direct = [(second + core, second + core), (first + core, first + core)]
        other = [first + 1 - core, second + 1 - core]
    else:
        direct = [
            (((chip + d) % chips) * 2 + core, ((chip + chips - d) % chips) * 2 + core)
            for d in range(1, chips)
        ]
        other = [((chip + chips - d) % chips) * 2 + 1 - core for d in range(1, chips)]
    sources = [s for _, s in direct]
    if forward:
        sources.append(across + core)
        other.append(across + 1 - core)

    high = c // 2
    beside = c + 1 - 2 * (c % 2)
    peers = [3 - c, (c + 2) % 4, beside]
    is_inner = (c == 1) | (c == 2)
    is_outer = (c == 0) | (c == 3)
    ends = [3 - 3 * high, 2 - high]

    loads = [
        pltpu.make_async_copy(v_hbm.at[0], v, load_sem.at[0]),
        pltpu.make_async_copy(
            omega_hbm.at[0, :, :WIDTH], omega.at[:, :WIDTH], load_sem.at[1]
        ),
        pltpu.make_async_copy(
            omega_hbm.at[0, :, WIDTH:], omega.at[:, WIDTH:], load_sem.at[2]
        ),
        pltpu.make_async_copy(map_hbm, maps, load_sem.at[3]),
        pltpu.make_async_copy(diag_hbm.at[0], diag, load_sem.at[4]),
        pltpu.make_async_copy(coupling_hbm.at[0], coupling, load_sem.at[5]),
        pltpu.make_async_copy(u_hbm.at[0], u, load_sem.at[6]),
    ]
    for load in loads[:2]:
        load.start()

    barrier = pltpu.get_barrier_semaphore()
    for to, _ in direct + [(partner, partner)]:
        pl.semaphore_signal(barrier, inc=1, device_id=(c, to), device_id_type=MESH)
    pl.semaphore_signal(barrier, inc=1, device_id=(beside, r), device_id_type=MESH)

    @pl.when(is_inner)
    def _():
        pl.semaphore_signal(barrier, inc=1, device_id=(3 - c, r), device_id_type=MESH)

    through = (0, last)
    summed = steps - len(through)

    def direct_step(s):
        return s in through

    def piece(s, source):
        size = block // 2
        base = (s % 2) * (depth // 2)
        return s // 2, pl.ds(pl.multiple_of(base + source * size, size), size)

    def rows_of(s, source):
        return gathered.at[piece(s, source)]

    def columns(g):
        return slice(g * WIDTH, (g + 1) * WIDTH)

    def project(first, end):
        mask = left_lanes(rank)
        size = block // 2
        values = []
        for i in range(leaves):
            rows = slice(i * leaf, (i + 1) * leaf)
            values.append(
                lax.dot_general(
                    v[rows, :], omega[rows, first * WIDTH : end * WIDTH], (((0,), (0,)), ((), ())),
                    preferred_element_type=jnp.float32,
                )
            )
        for i in range(leaves):
            mine[0, i * rank : (i + 1) * rank, first * WIDTH : end * WIDTH] = values[i].astype(
                jnp.bfloat16
            )
        for i in range(leaves // 2):
            for g in range(first, end):
                cols = columns(g - first)
                low, up = values[i][:, cols], pltpu.roll(values[i + leaves // 2][:, cols], HALF, 1)
                at = pl.multiple_of(r * size + i * rank, rank)
                gathered[g, pl.ds(at, rank), :] = jnp.where(mask, low, up).astype(jnp.bfloat16)
                at = pl.multiple_of(depth // 2 + r * size + i * rank, rank)
                gathered[g, pl.ds(at, rank), :] = jnp.where(mask, up, low).astype(jnp.bfloat16)

    def remote(src, dst, send, recv, to):
        return pltpu.make_async_remote_copy(
            src_ref=src, dst_ref=dst, send_sem=send, recv_sem=recv,
            device_id=to, device_id_type=MESH,
        )

    def ici(t, s):
        at = rows_of(s, r)
        return remote(at, at, ici_send.at[t], ici_recv.at[t, s], (c, direct[t][0]))

    def ici_in(t, s):
        at = rows_of(s, direct[t][1])
        return remote(at, at, ici_send.at[t], ici_recv.at[t, s], (c, direct[t][0]))

    def fwd(s):
        at = rows_of(s, direct[0][1])
        return remote(at, at, fwd_send, fwd_recv.at[s], (c, direct[1][0]))

    def fwd_in(s):
        at = rows_of(s, sources[-1])
        return remote(at, at, fwd_send, fwd_recv.at[s], (c, direct[1][0]))

    def core_kind(t):
        return 1 if forward and t == 2 else 0

    def across_core(t, s, who):
        at = rows_of(s, who[t])
        return remote(at, at, core_send, core_recv.at[core_kind(t), s], (c, partner))

    def to_peer(j, s):
        return remote(
            update.at[s, peers[j]], peer_in.at[s, j],
            peer_send.at[j],
            near_recv.at[s] if j == 2 else peer_recv.at[through.index(s), j],
            (peers[j], r),
        )

    def to_inner(s):
        return remote(
            update.at[s, pl.ds(2 - 2 * high, 2)], inner_in.at[s],
            inner_send, inner_recv.at[s], (beside, r),
        )

    def to_far(e, s):
        return remote(
            sums.at[s, e], far_in.at[s], far_send, far_recv.at[s], (ends[e], r)
        )

    def to_partner():
        return remote(mine.at[0], mine.at[1], mine_send, mine_recv, (c, partner))

    def map_to_peer(j):
        return remote(
            slots.at[peers[j]], slots_in.at[j], map_send.at[0], map_recv.at[0], (peers[j], r)
        )

    def map_to_inner(e):
        return remote(
            slots.at[ends[e]], inner_slots.at[e],
            map_send.at[1], map_recv.at[1], (beside, r),
        )

    def from_partner(s, kind, count):
        at = gathered.at[0, pl.ds(0, count * (block // 2))]
        remote(at, at, core_send, core_recv.at[kind, s], (c, partner)).wait_recv()

    def start(copy):
        copy.start()

    def send_own(t, s):
        if s <= last:
            start(ici(t, s))

    def arrive(t, s):
        if s <= last:
            ici_in(t, s).wait_recv()
            if forward and t == 0:
                start(fwd(s))
            start(across_core(t, s, sources))

    def arrive_across(s):
        fwd_in(s).wait_recv()
        start(across_core(len(sources) - 1, s, sources))

    def part(s, source, fresh=False):
        k = s % 2
        g, at = piece(s, source)
        value = gathered[g, at, :]
        size = block // 2
        for h in range(2):
            cols = pl.ds(pl.multiple_of(source * block + h * size, size), size)
            term = dot(coupling[:, cols], value)
            total[k, h] = term if fresh else total[k, h] + term

    def settle(s):
        k = s % 2
        mask = left_lanes(block)
        known = near_total[:, columns(s // 2)]
        known = jnp.where(mask, known, 0.0) if k == 0 else jnp.where(mask, 0.0, known)
        mixed = jnp.where(mask, total[k, k], total[k, 1 - k]) + known
        coupled[k] = (mixed + pltpu.roll(mixed, HALF, 1)).astype(jnp.bfloat16)

    def local_rows(i):
        value = dot(diag[i], omega[i * leaf : (i + 1) * leaf, :])
        mask = left_lanes(leaf // 2)
        for g in range(groups):
            low = value[: leaf // 2, columns(g)]
            up = pltpu.roll(value[leaf // 2 :, columns(g)], HALF, 1)
            local_part[2 * g, i] = jnp.where(mask, low, up)
            local_part[2 * g + 1, i] = jnp.where(mask, up, low)

    def finish(s):
        settle(s)
        mask = left_lanes(leaf // 2)
        whole = direct_step(s)
        for e, i in enumerate((peers if whole else ends + [beside]) + [c]):
            rows = pl.ds(pl.multiple_of(i * leaf, leaf), leaf)
            at = pl.ds(pl.multiple_of(i * rank, rank), rank)
            value = dot(u[rows, :], coupled[s % 2, at, :])
            low, up = value[: leaf // 2], value[leaf // 2 :]
            mixed = jnp.where(mask, low, up) if s % 2 == 0 else jnp.where(mask, up, low)
            update[s, i] = (mixed + local_part[s, i]).astype(jnp.bfloat16)
            if whole and e < 3:
                start(to_peer(e, s))
            elif e == 1:
                @pl.when(is_outer)
                def _():
                    to_inner(s).start()
            elif e == 2:
                start(to_peer(2, s))

    def spread(value, slot, s):
        value = value.astype(jnp.float32)
        turned = pltpu.roll(value, HALF, 1)
        lanes = lax.broadcasted_iota(jnp.int32, (1, WIDTH), 1)
        main = lanes < HALF if s % 2 == 0 else lanes >= HALF
        s0, s1 = slot[0:1, :], slot[4:5, :]
        held, swapped = jnp.where(main, s0, s1), jnp.where(main, s1, s0)
        want = jnp.where(main, 0.0, 1.0)
        pair = jnp.where(held == want, value, jnp.where(swapped == want, turned, 0.0))
        third = jnp.where(held == 2.0, value, jnp.where(swapped == 2.0, turned, 0.0))
        quarter = leaf // 4
        mask = left_lanes(quarter)
        top, bottom = third[:quarter], third[quarter:]
        folded = jnp.where(mask, top, bottom) if s % 2 == 0 else jnp.where(mask, bottom, top)
        return jnp.concatenate([pair, folded], axis=0)

    def combine(s):
        if s >= 0 and not direct_step(s):
            @pl.when(is_inner)
            def _():
                to_inner(s).wait_recv()
                for e in range(2):
                    value = spread(update[s, ends[e]], slots[ends[e]], s) + spread(
                        inner_in[s, ends[e] - (2 - 2 * high)], inner_slots[e], s
                    )
                    sums[s, e] = value.astype(jnp.bfloat16)
                    to_far(e, s).start()

    def final(s):
        if s < 0:
            return
        value = spread(update[s, c], slots[c], s)
        if direct_step(s):
            for j in reversed(range(3)):
                to_peer(j, s).wait_recv()
                value = value + spread(peer_in[s, j], slots_in[j], s)
        else:
            to_peer(2, s).wait_recv()
            value = value + spread(peer_in[s, 2], slots_in[2], s)
            to_far(0, s).wait_recv()
            value = value + far_in[s].astype(jnp.float32)
        if s % 2 == 0:
            halves[...] = value
        else:
            cols, size, quarter = columns(s // 2), leaf // 2, leaf // 4
            mask = left_lanes(3 * quarter)
            before = halves[...]
            straight = jnp.where(mask, before, value)
            turned = pltpu.roll(jnp.where(mask, value, before), HALF, 1)
            out[0, :, cols] = straight[:size]
            out[1, :, cols] = turned[:size]
            out[2, :quarter, cols] = straight[size:]
            out[2, quarter:, cols] = turned[size:]

    loads[0].wait()
    loads[1].wait()
    for load in loads[2:]:
        load.start()
    project(0, 1)

    @pl.when(is_outer)
    def _():
        pl.semaphore_wait(barrier, len(direct) + 2)

    @pl.when(is_inner)
    def _():
        pl.semaphore_wait(barrier, len(direct) + 3)

    for t in reversed(range(len(direct))):
        send_own(t, 0)
    if forward:
        send_own(0, 1)
    loads[2].wait()
    project(1, groups)
    to_partner().start()
    for s in range(1, AHEAD):
        send_own(0, s + 1 if forward else s)
        if not forward:
            for t in range(1, len(direct)):
                send_own(t, s)

    def take_maps():
        remote(slots_in, slots_in, map_send.at[0], map_recv.at[0], (beside, r)).wait_recv()

        @pl.when(is_inner)
        def _():
            remote(
                inner_slots, inner_slots, map_send.at[1], map_recv.at[1], (beside, r)
            ).wait_recv()

    def take(s):
        arrive(0, s)
        send_own(1, s + 1)
        send_own(0, s + 1 + AHEAD)

    loads[3].wait()
    for i in range(leaves):
        for b in range(2):
            slot = maps[0, 2 * i + b] - 3 * (r * leaves + i)
            slots[i, 4 * b : 4 * b + 4, :] = jnp.full((4, WIDTH), slot, jnp.int32).astype(
                jnp.float32
            )

    @pl.when(is_inner)
    def _():
        pl.semaphore_signal(ready, inc=1, device_id=(3 - c, r), device_id_type=MESH)
        pl.semaphore_wait(ready, 1)
        pl.semaphore_signal(ready, inc=1, device_id=(beside, r), device_id_type=MESH)

    @pl.when(is_outer)
    def _():
        pl.semaphore_wait(ready, 1)

    for j in range(len(peers)):
        map_to_peer(j).start()

    @pl.when(is_outer)
    def _():
        for e in range(2):
            map_to_inner(e).start()

    if forward:
        take(0)
        arrive(1, 0)
        take(1)
    for load in loads[4:]:
        load.wait()
    for i in range(leaves):
        local_rows(i)
    near_total[...] = dot(coupling[:, pl.ds(pl.multiple_of(r * block, block), block)], mine[0])
    to_partner().wait_recv()
    near_total[...] += dot(
        coupling[:, pl.ds(pl.multiple_of(partner * block, block), block)], mine[1]
    )
    if forward:
        part(0, sources[0], True)
        part(0, sources[1])

    for s in range(steps):
        if forward:
            arrive_across(s)
            from_partner(s, 0, 2)
            for source in (other[0], other[1], sources[2]):
                part(s, source)
            if s + 2 <= last:
                take(s + 2)
            if s == 1:
                take_maps()
            combine(s - LAG)
            arrive(1, s + 1)
            if s < last:
                part(s + 1, sources[0], True)
                part(s + 1, sources[1])
            final(s - DONE)
            from_partner(s, 1, 1)
            part(s, other[2])
        else:
            for t in range(len(direct)):
                arrive(t, s)
                send_own(t, s + AHEAD)
            from_partner(s, 0, len(other))
            if s == 1:
                take_maps()
            combine(s - LAG)
            final(s - DONE)

            def more(d, carry, s=s):
                for e in range(2):
                    part(s, (chip + d) % chips * 2 + e)
                return carry

            part(s, (chip + 1) % chips * 2, True)
            part(s, (chip + 1) % chips * 2 + 1)
            lax.fori_loop(2, chips, more, 0)
        finish(s)
    for s in range(last - LAG + 1, steps):
        combine(s)
    for s in range(last - DONE + 1, steps):
        final(s)

    def drain(ref, sem):
        remote(ref, ref, sem, map_recv.at[0], (beside, r)).wait_send()

    for t in range(len(direct)):
        drain(gathered.at[:, pl.ds(0, block)], ici_send.at[t])
    if forward:
        drain(gathered.at[:, pl.ds(0, block)], fwd_send)
    drain(gathered.at[:, pl.ds(0, len(sources) * block)], core_send)
    to_partner().wait_send()
    for j in range(2):
        drain(update.at[0, pl.ds(0, len(through))], peer_send.at[j])
    drain(update.at[:, 0], peer_send.at[2])
    drain(slots.at[pl.ds(0, len(peers))], map_send.at[0])

    @pl.when(is_outer)
    def _():
        drain(slots.at[pl.ds(0, 2)], map_send.at[1])
        drain(update.at[pl.ds(0, summed), pl.ds(0, 2)], inner_send)

    @pl.when(is_inner)
    def _():
        drain(sums.at[pl.ds(0, summed)], far_send)


def write(value, out, sem):
    copies = [
        pltpu.make_async_copy(value.at[q], out.at[q], sem.at[q]) for q in range(out.shape[0])
    ]
    for copy in copies:
        copy.start()
    for copy in copies:
        copy.wait()


def solution(mesh):
    n_child, n_rows = mesh.shape["child"], mesh.shape["rows"]

    def on_device(omega, leaf_diag, leaf_u, leaf_v, coupling, child_map):
        leaves, leaf = leaf_diag.shape[1], leaf_diag.shape[2]
        rank, samples = leaf_u.shape[2], omega.shape[2]
        groups = samples // WIDTH
        steps = 2 * groups
        block, depth = coupling.shape[1], coupling.shape[2]
        chips = n_rows // 2
        direct = 2 if chips == 4 else chips - 1
        everyone = 1 + direct + (chips == 4)
        peers = n_child - 1
        vmem = pltpu.VMEM
        bf16, f32 = jnp.bfloat16, jnp.float32
        dma = pltpu.SemaphoreType.DMA
        anywhere = pl.BlockSpec(memory_space=pl.ANY)
        shape = (3, leaf // 2, samples)
        value = pl.pallas_call(
            functools.partial(kernel, n_child, n_rows),
            out_shape=vmem(shape, f32),
            in_specs=[anywhere] * 6,
            out_specs=pl.BlockSpec(memory_space=vmem),
            scratch_shapes=[
                vmem((leaves * leaf, samples), bf16),
                vmem((leaves * leaf, rank), bf16),
                vmem((leaves, leaf, leaf), bf16),
                vmem((leaves * leaf, rank), bf16),
                vmem((block, depth), bf16),
                vmem((groups, depth, WIDTH), bf16),
                vmem((2, block, samples), bf16),
                vmem((block, samples), f32),
                vmem((steps, leaves, leaf // 2, WIDTH), f32),
                vmem((2, 2, block, WIDTH), f32),
                vmem((2, block, WIDTH), bf16),
                vmem((steps, leaves, leaf // 2, WIDTH), bf16),
                vmem((steps, 2, 3 * leaf // 4, WIDTH), bf16),
                vmem((steps, peers, leaf // 2, WIDTH), bf16),
                vmem((steps, 2, leaf // 2, WIDTH), bf16),
                vmem((steps, 3 * leaf // 4, WIDTH), bf16),
                vmem((3 * leaf // 4, WIDTH), f32),
                pltpu.SMEM(child_map.shape, jnp.int32),
                vmem((leaves, 8, WIDTH), f32),
                vmem((peers, 8, WIDTH), f32),
                vmem((2, 8, WIDTH), f32),
                dma((7,)),
                dma((direct,)),
                dma((direct, steps)),
                dma,
                dma((steps,)),
                dma,
                dma((2, steps)),
                dma,
                dma,
                dma((peers,)),
                dma((steps,)),
                dma((2, 2)),
                dma,
                dma((steps,)),
                dma,
                dma((steps,)),
                dma((2,)),
                dma((2,)),
                pltpu.SemaphoreType.REGULAR,
            ],
            compiler_params=pltpu.CompilerParams(
                collective_id=0, has_side_effects=True, vmem_limit_bytes=52 * 1024 * 1024
            ),
        )(*[
            pltpu.with_memory_space_constraint(array, pltpu.HBM)
            for array in (omega, leaf_v, child_map, leaf_diag, leaf_u, coupling)
        ])
        value = pltpu.with_memory_space_constraint(value, vmem)
        return pl.pallas_call(
            write,
            out_shape=jax.ShapeDtypeStruct(shape, f32),
            in_specs=[pl.BlockSpec(memory_space=vmem)],
            out_specs=anywhere,
            scratch_shapes=[dma((3,))],
        )(value)

    placed = (
        P("child", "rows", None),
        P("child", "rows", None, None),
        P("child", "rows", None),
        P("child", "rows", None),
        P("child", "rows", None),
        P("child", "rows"),
    )
    return jax.shard_map(
        on_device,
        mesh=mesh,
        in_specs=placed,
        out_specs=P(None, ("child", "rows"), None),
        check_vma=False,
    )
```

```python
import functools

import jax
import jax.numpy as jnp
from jax import lax
from jax.experimental import pallas as pl
from jax.experimental.pallas import tpu as pltpu
from jax.sharding import PartitionSpec as P

MESH = pl.DeviceIdType.MESH
WIDTH = 128
HALF = WIDTH // 2
AHEAD = 2
LAG = 2
DONE = 6
LATE = 2


def dot(a, b):
    return jnp.dot(a, b, preferred_element_type=jnp.float32)


def left_lanes(rows):
    return lax.broadcasted_iota(jnp.int32, (rows, WIDTH), 1) < HALF


def kernel(
    n_child, n_rows, omega_hbm, v_hbm, map_hbm, diag_hbm, u_hbm, coupling_hbm, out,
    omega, v, diag, u, coupling, gathered, mine, near_total, local_part, total, coupled,
    update, sums, peer_in, inner_in, far_in, halves, maps, slots, slots_in, inner_slots,
    load_sem, ici_send, ici_recv, fwd_send, fwd_recv, core_send, core_recv, mine_send, mine_recv,
    peer_send, near_recv, peer_recv, inner_send, inner_recv, far_send, far_recv,
    map_send, map_recv, ready,
):
    groups, depth = gathered.shape[0], gathered.shape[1]
    leaves, leaf = diag.shape[0], diag.shape[1]
    rank = u.shape[1]
    block = leaves * rank
    chips = n_rows // 2
    steps = 2 * groups
    last = steps - 1
    c = lax.axis_index("child")
    r = lax.axis_index("rows")
    chip, core = r // 2, r % 2
    partner = chip * 2 + 1 - core

    forward = chips == 4
    if forward:
        x, y = chip % 2, chip // 2
        x_near = (y * 2 + 1 - x) * 2
        y_near = ((1 - y) * 2 + x) * 2
        first = x_near * (1 - core) + y_near * core
        second = y_near * (1 - core) + x_near * core
        across = ((1 - y) * 2 + 1 - x) * 2
        direct = [(second + core, second + core), (first + core, first + core)]
        other = [first + 1 - core, second + 1 - core]
    else:
        direct = [
            (((chip + d) % chips) * 2 + core, ((chip + chips - d) % chips) * 2 + core)
            for d in range(1, chips)
        ]
        other = [((chip + chips - d) % chips) * 2 + 1 - core for d in range(1, chips)]
    sources = [s for _, s in direct]
    if forward:
        sources.append(across + core)
        other.append(across + 1 - core)

    high = c // 2
    beside = c + 1 - 2 * (c % 2)
    peers = [3 - c, (c + 2) % 4, beside]
    is_inner = (c == 1) | (c == 2)
    is_outer = (c == 0) | (c == 3)
    ends = [3 - 3 * high, 2 - high]

    loads = [
        pltpu.make_async_copy(v_hbm.at[0], v, load_sem.at[0]),
        pltpu.make_async_copy(
            omega_hbm.at[0, :, :WIDTH], omega.at[:, :WIDTH], load_sem.at[1]
        ),
        pltpu.make_async_copy(
            omega_hbm.at[0, :, WIDTH:], omega.at[:, WIDTH:], load_sem.at[2]
        ),
        pltpu.make_async_copy(map_hbm, maps, load_sem.at[3]),
        pltpu.make_async_copy(diag_hbm.at[0], diag, load_sem.at[4]),
        pltpu.make_async_copy(coupling_hbm.at[0], coupling, load_sem.at[5]),
        pltpu.make_async_copy(u_hbm.at[0], u, load_sem.at[6]),
    ]
    for load in loads[:2]:
        load.start()

    barrier = pltpu.get_barrier_semaphore()
    for to, _ in direct + [(partner, partner)]:
        pl.semaphore_signal(barrier, inc=1, device_id=(c, to), device_id_type=MESH)
    pl.semaphore_signal(barrier, inc=1, device_id=(beside, r), device_id_type=MESH)

    @pl.when(is_inner)
    def _():
        pl.semaphore_signal(barrier, inc=1, device_id=(3 - c, r), device_id_type=MESH)

    through = (0,)
    summed = steps - len(through)

    def direct_step(s):
        return s in through

    def piece(s, source):
        size = block // 2
        base = (s % 2) * (depth // 2)
        return s // 2, pl.ds(pl.multiple_of(base + source * size, size), size)

    def rows_of(s, source):
        return gathered.at[piece(s, source)]

    def columns(g):
        return slice(g * WIDTH, (g + 1) * WIDTH)

    def project(first, end):
        mask = left_lanes(rank)
        size = block // 2
        values = []
        for i in range(leaves):
            rows = slice(i * leaf, (i + 1) * leaf)
            values.append(
                lax.dot_general(
                    v[rows, :], omega[rows, first * WIDTH : end * WIDTH], (((0,), (0,)), ((), ())),
                    preferred_element_type=jnp.float32,
                )
            )
        for i in range(leaves):
            mine[0, i * rank : (i + 1) * rank, first * WIDTH : end * WIDTH] = values[i].astype(
                jnp.bfloat16
            )
        for i in range(leaves // 2):
            for g in range(first, end):
                cols = columns(g - first)
                low, up = values[i][:, cols], pltpu.roll(values[i + leaves // 2][:, cols], HALF, 1)
                at = pl.multiple_of(r * size + i * rank, rank)
                gathered[g, pl.ds(at, rank), :] = jnp.where(mask, low, up).astype(jnp.bfloat16)
                at = pl.multiple_of(depth // 2 + r * size + i * rank, rank)
                gathered[g, pl.ds(at, rank), :] = jnp.where(mask, up, low).astype(jnp.bfloat16)

    def remote(src, dst, send, recv, to):
        return pltpu.make_async_remote_copy(
            src_ref=src, dst_ref=dst, send_sem=send, recv_sem=recv,
            device_id=to, device_id_type=MESH,
        )

    def ici(t, s):
        at = rows_of(s, r)
        return remote(at, at, ici_send.at[t], ici_recv.at[t, s], (c, direct[t][0]))

    def ici_in(t, s):
        at = rows_of(s, direct[t][1])
        return remote(at, at, ici_send.at[t], ici_recv.at[t, s], (c, direct[t][0]))

    def fwd(s):
        at = rows_of(s, direct[0][1])
        return remote(at, at, fwd_send, fwd_recv.at[s], (c, direct[1][0]))

    def fwd_in(s):
        at = rows_of(s, sources[-1])
        return remote(at, at, fwd_send, fwd_recv.at[s], (c, direct[1][0]))

    def core_kind(t):
        return 1 if forward and t == 2 else 0

    def across_core(t, s, who):
        at = rows_of(s, who[t])
        return remote(at, at, core_send, core_recv.at[core_kind(t), s], (c, partner))

    def to_peer(j, s):
        return remote(
            update.at[s, peers[j]], peer_in.at[s, j],
            peer_send.at[j],
            near_recv.at[s] if j == 2 else peer_recv.at[through.index(s), j],
            (peers[j], r),
        )

    def to_inner(s):
        return remote(
            update.at[s, pl.ds(2 - 2 * high, 2)], inner_in.at[s],
            inner_send, inner_recv.at[s], (beside, r),
        )

    def to_far(e, s):
        return remote(
            sums.at[s, e], far_in.at[s], far_send, far_recv.at[s], (ends[e], r)
        )

    def to_partner():
        return remote(mine.at[0], mine.at[1], mine_send, mine_recv, (c, partner))

    def map_to_peer(j):
        return remote(
            slots.at[peers[j]], slots_in.at[j], map_send.at[0], map_recv.at[0], (peers[j], r)
        )

    def map_to_inner(e):
        return remote(
            slots.at[ends[e]], inner_slots.at[e],
            map_send.at[1], map_recv.at[1], (beside, r),
        )

    def from_partner(s, kind, count):
        at = gathered.at[0, pl.ds(0, count * (block // 2))]
        remote(at, at, core_send, core_recv.at[kind, s], (c, partner)).wait_recv()

    def start(copy):
        copy.start()

    def send_own(t, s):
        if s <= last:
            start(ici(t, s))

    def arrive(t, s):
        if s <= last:
            ici_in(t, s).wait_recv()
            if forward and t == 0:
                start(fwd(s))
            start(across_core(t, s, sources))

    def arrive_across(s):
        fwd_in(s).wait_recv()
        start(across_core(len(sources) - 1, s, sources))

    def part(s, source, fresh=False):
        k = s % 2
        g, at = piece(s, source)
        value = gathered[g, at, :]
        size = block // 2
        for h in range(2):
            cols = pl.ds(pl.multiple_of(source * block + h * size, size), size)
            term = dot(coupling[:, cols], value)
            total[k, h] = term if fresh else total[k, h] + term

    def settle(s):
        k = s % 2
        mask = left_lanes(block)
        known = near_total[:, columns(s // 2)]
        known = jnp.where(mask, known, 0.0) if k == 0 else jnp.where(mask, 0.0, known)
        mixed = jnp.where(mask, total[k, k], total[k, 1 - k]) + known
        coupled[k] = (mixed + pltpu.roll(mixed, HALF, 1)).astype(jnp.bfloat16)

    def local_rows(i):
        value = dot(diag[i], omega[i * leaf : (i + 1) * leaf, :])
        mask = left_lanes(leaf // 2)
        for g in range(groups):
            low = value[: leaf // 2, columns(g)]
            up = pltpu.roll(value[leaf // 2 :, columns(g)], HALF, 1)
            local_part[2 * g, i] = jnp.where(mask, low, up)
            local_part[2 * g + 1, i] = jnp.where(mask, up, low)

    def near_later(s):
        if s >= 0 and not direct_step(s):
            start(to_peer(2, s))

    def finish(s):
        settle(s)
        mask = left_lanes(leaf // 2)
        whole = direct_step(s)
        for e, i in enumerate((peers if whole else ends + [beside]) + [c]):
            rows = pl.ds(pl.multiple_of(i * leaf, leaf), leaf)
            at = pl.ds(pl.multiple_of(i * rank, rank), rank)
            value = dot(u[rows, :], coupled[s % 2, at, :])
            low, up = value[: leaf // 2], value[leaf // 2 :]
            mixed = jnp.where(mask, low, up) if s % 2 == 0 else jnp.where(mask, up, low)
            update[s, i] = (mixed + local_part[s, i]).astype(jnp.bfloat16)
            if whole and e < 3:
                start(to_peer(e, s))
            elif e == 1:
                @pl.when(is_outer)
                def _():
                    to_inner(s).start()
            elif e == 2:
                near_later(s - LATE)

    def spread(value, slot, s):
        value = value.astype(jnp.float32)
        turned = pltpu.roll(value, HALF, 1)
        lanes = lax.broadcasted_iota(jnp.int32, (1, WIDTH), 1)
        main = lanes < HALF if s % 2 == 0 else lanes >= HALF
        s0, s1 = slot[0:1, :], slot[4:5, :]
        held, swapped = jnp.where(main, s0, s1), jnp.where(main, s1, s0)
        want = jnp.where(main, 0.0, 1.0)
        pair = jnp.where(held == want, value, jnp.where(swapped == want, turned, 0.0))
        third = jnp.where(held == 2.0, value, jnp.where(swapped == 2.0, turned, 0.0))
        quarter = leaf // 4
        mask = left_lanes(quarter)
        top, bottom = third[:quarter], third[quarter:]
        folded = jnp.where(mask, top, bottom) if s % 2 == 0 else jnp.where(mask, bottom, top)
        return jnp.concatenate([pair, folded], axis=0)

    def combine(s):
        if s >= 0 and not direct_step(s):
            @pl.when(is_inner)
            def _():
                to_inner(s).wait_recv()
                for e in range(2):
                    value = spread(update[s, ends[e]], slots[ends[e]], s) + spread(
                        inner_in[s, ends[e] - (2 - 2 * high)], inner_slots[e], s
                    )
                    sums[s, e] = value.astype(jnp.bfloat16)
                    to_far(e, s).start()

    def final(s):
        if s < 0:
            return
        value = spread(update[s, c], slots[c], s)
        if direct_step(s):
            for j in reversed(range(3)):
                to_peer(j, s).wait_recv()
                value = value + spread(peer_in[s, j], slots_in[j], s)
        else:
            to_peer(2, s).wait_recv()
            value = value + spread(peer_in[s, 2], slots_in[2], s)
            to_far(0, s).wait_recv()
            value = value + far_in[s].astype(jnp.float32)
        if s % 2 == 0:
            halves[...] = value
        else:
            cols, size, quarter = columns(s // 2), leaf // 2, leaf // 4
            mask = left_lanes(3 * quarter)
            before = halves[...]
            straight = jnp.where(mask, before, value)
            turned = pltpu.roll(jnp.where(mask, value, before), HALF, 1)
            out[0, :, cols] = straight[:size]
            out[1, :, cols] = turned[:size]
            out[2, :quarter, cols] = straight[size:]
            out[2, quarter:, cols] = turned[size:]

    loads[0].wait()
    loads[1].wait()
    for load in loads[2:]:
        load.start()
    project(0, 1)

    @pl.when(is_outer)
    def _():
        pl.semaphore_wait(barrier, len(direct) + 2)

    @pl.when(is_inner)
    def _():
        pl.semaphore_wait(barrier, len(direct) + 3)

    for t in reversed(range(len(direct))):
        send_own(t, 0)
    if forward:
        send_own(0, 1)
    loads[2].wait()
    project(1, groups)
    to_partner().start()
    for s in range(1, AHEAD):
        send_own(0, s + 1 if forward else s)
        if not forward:
            for t in range(1, len(direct)):
                send_own(t, s)

    def take_maps():
        remote(slots_in, slots_in, map_send.at[0], map_recv.at[0], (beside, r)).wait_recv()

        @pl.when(is_inner)
        def _():
            remote(
                inner_slots, inner_slots, map_send.at[1], map_recv.at[1], (beside, r)
            ).wait_recv()

    def take(s):
        arrive(0, s)
        send_own(1, s + 1)
        send_own(0, s + 1 + AHEAD)

    loads[3].wait()
    for i in range(leaves):
        for b in range(2):
            slot = maps[0, 2 * i + b] - 3 * (r * leaves + i)
            slots[i, 4 * b : 4 * b + 4, :] = jnp.full((4, WIDTH), slot, jnp.int32).astype(
                jnp.float32
            )

    @pl.when(is_inner)
    def _():
        pl.semaphore_signal(ready, inc=1, device_id=(3 - c, r), device_id_type=MESH)
        pl.semaphore_wait(ready, 1)
        pl.semaphore_signal(ready, inc=1, device_id=(beside, r), device_id_type=MESH)

    @pl.when(is_outer)
    def _():
        pl.semaphore_wait(ready, 1)

    for j in range(len(peers)):
        map_to_peer(j).start()

    @pl.when(is_outer)
    def _():
        for e in range(2):
            map_to_inner(e).start()

    if forward:
        take(0)
        arrive(1, 0)
        take(1)
    for load in loads[4:]:
        load.wait()
    for i in range(leaves):
        local_rows(i)
    near_total[...] = dot(coupling[:, pl.ds(pl.multiple_of(r * block, block), block)], mine[0])
    to_partner().wait_recv()
    near_total[...] += dot(
        coupling[:, pl.ds(pl.multiple_of(partner * block, block), block)], mine[1]
    )
    if forward:
        part(0, sources[0], True)
        part(0, sources[1])

    for s in range(steps):
        if forward:
            arrive_across(s)
            from_partner(s, 0, 2)
            for source in (other[0], other[1], sources[2]):
                part(s, source)
            if s + 2 <= last:
                take(s + 2)
            if s == 1:
                take_maps()
            combine(s - LAG)
            arrive(1, s + 1)
            if s < last:
                part(s + 1, sources[0], True)
                part(s + 1, sources[1])
            final(s - DONE)
            from_partner(s, 1, 1)
            part(s, other[2])
        else:
            for t in range(len(direct)):
                arrive(t, s)
                send_own(t, s + AHEAD)
            from_partner(s, 0, len(other))
            if s == 1:
                take_maps()
            combine(s - LAG)
            final(s - DONE)

            def more(d, carry, s=s):
                for e in range(2):
                    part(s, (chip + d) % chips * 2 + e)
                return carry

            part(s, (chip + 1) % chips * 2, True)
            part(s, (chip + 1) % chips * 2 + 1)
            lax.fori_loop(2, chips, more, 0)
        finish(s)
    for s in range(last - LATE + 1, steps):
        near_later(s)
    for s in range(last - LAG + 1, last):
        combine(s)
    for s in range(last - DONE + 1, last - 2):
        final(s)
    combine(last)
    for s in range(last - 2, steps):
        final(s)

    def drain(ref, sem):
        remote(ref, ref, sem, map_recv.at[0], (beside, r)).wait_send()

    for t in range(len(direct)):
        drain(gathered.at[:, pl.ds(0, block)], ici_send.at[t])
    if forward:
        drain(gathered.at[:, pl.ds(0, block)], fwd_send)
    drain(gathered.at[:, pl.ds(0, len(sources) * block)], core_send)
    to_partner().wait_send()
    for j in range(2):
        drain(gathered.at[0, pl.ds(0, 128*len(through))], peer_send.at[j])
    drain(update.at[:, 0], peer_send.at[2])
    drain(slots.at[pl.ds(0, len(peers))], map_send.at[0])

    @pl.when(is_outer)
    def _():
        drain(slots.at[pl.ds(0, 2)], map_send.at[1])
        drain(update.at[pl.ds(0, summed), pl.ds(0, 2)], inner_send)

    @pl.when(is_inner)
    def _():
        drain(sums.at[pl.ds(0, summed)], far_send)


def write(value, out, sem):
    copies = [
        pltpu.make_async_copy(value.at[q], out.at[q], sem.at[q]) for q in range(out.shape[0])
    ]
    for copy in copies:
        copy.start()
    for copy in copies:
        copy.wait()


def solution(mesh):
    n_child, n_rows = mesh.shape["child"], mesh.shape["rows"]

    def on_device(omega, leaf_diag, leaf_u, leaf_v, coupling, child_map):
        leaves, leaf = leaf_diag.shape[1], leaf_diag.shape[2]
        rank, samples = leaf_u.shape[2], omega.shape[2]
        groups = samples // WIDTH
        steps = 2 * groups
        block, depth = coupling.shape[1], coupling.shape[2]
        chips = n_rows // 2
        direct = 2 if chips == 4 else chips - 1
        everyone = 1 + direct + (chips == 4)
        peers = n_child - 1
        vmem = pltpu.VMEM
        bf16, f32 = jnp.bfloat16, jnp.float32
        dma = pltpu.SemaphoreType.DMA
        anywhere = pl.BlockSpec(memory_space=pl.ANY)
        shape = (3, leaf // 2, samples)
        value = pl.pallas_call(
            functools.partial(kernel, n_child, n_rows),
            out_shape=vmem(shape, f32),
            in_specs=[anywhere] * 6,
            out_specs=pl.BlockSpec(memory_space=vmem),
            scratch_shapes=[
                vmem((leaves * leaf, samples), bf16),
                vmem((leaves * leaf, rank), bf16),
                vmem((leaves, leaf, leaf), bf16),
                vmem((leaves * leaf, rank), bf16),
                vmem((block, depth), bf16),
                vmem((groups, depth, WIDTH), bf16),
                vmem((2, block, samples), bf16),
                vmem((block, samples), f32),
                vmem((steps, leaves, leaf // 2, WIDTH), f32),
                vmem((2, 2, block, WIDTH), f32),
                vmem((2, block, WIDTH), bf16),
                vmem((steps, leaves, leaf // 2, WIDTH), bf16),
                vmem((steps, 2, 3 * leaf // 4, WIDTH), bf16),
                vmem((steps, peers, leaf // 2, WIDTH), bf16),
                vmem((steps, 2, leaf // 2, WIDTH), bf16),
                vmem((steps, 3 * leaf // 4, WIDTH), bf16),
                vmem((3 * leaf // 4, WIDTH), f32),
                pltpu.SMEM(child_map.shape, jnp.int32),
                vmem((leaves, 8, WIDTH), f32),
                vmem((peers, 8, WIDTH), f32),
                vmem((2, 8, WIDTH), f32),
                dma((7,)),
                dma((direct,)),
                dma((direct, steps)),
                dma,
                dma((steps,)),
                dma,
                dma((2, steps)),
                dma,
                dma,
                dma((peers,)),
                dma((steps,)),
                dma((8, 2)),
                dma,
                dma((steps,)),
                dma,
                dma((steps,)),
                dma((2,)),
                dma((2,)),
                pltpu.SemaphoreType.REGULAR,
            ],
            compiler_params=pltpu.CompilerParams(
                collective_id=0, has_side_effects=True, vmem_limit_bytes=52 * 1024 * 1024
            ),
        )(*[
            pltpu.with_memory_space_constraint(array, pltpu.HBM)
            for array in (omega, leaf_v, child_map, leaf_diag, leaf_u, coupling)
        ])
        value = pltpu.with_memory_space_constraint(value, vmem)
        return pl.pallas_call(
            write,
            out_shape=jax.ShapeDtypeStruct(shape, f32),
            in_specs=[pl.BlockSpec(memory_space=vmem)],
            out_specs=anywhere,
            scratch_shapes=[dma((3,))],
        )(value)

    placed = (
        P("child", "rows", None),
        P("child", "rows", None, None),
        P("child", "rows", None),
        P("child", "rows", None),
        P("child", "rows", None),
        P("child", "rows"),
    )
    return jax.shard_map(
        on_device,
        mesh=mesh,
        in_specs=placed,
        out_specs=P(None, ("child", "rows"), None),
        check_vma=False,
    )
```

```python
import functools

import jax
import jax.numpy as jnp
from jax import lax
from jax.experimental import pallas as pl
from jax.experimental.pallas import tpu as pltpu
from jax.sharding import PartitionSpec as P

MESH = pl.DeviceIdType.MESH
WIDTH = 128
HALF = WIDTH // 2
AHEAD = 2
LAG = 2
DONE = 6
LATE = 2


def dot(a, b):
    return jnp.dot(a, b, preferred_element_type=jnp.float32)


def left_lanes(rows):
    return lax.broadcasted_iota(jnp.int32, (rows, WIDTH), 1) < HALF


def kernel(
    n_child, n_rows, omega_hbm, v_hbm, map_hbm, diag_hbm, u_hbm, coupling_hbm, out,
    omega, v, diag, u, coupling, gathered, mine, near_total, local_part, total, coupled,
    update, sums, peer_in, inner_in, far_in, halves, maps, slots, slots_in, inner_slots,
    load_sem, ici_send, ici_recv, fwd_send, fwd_recv, core_send, core_recv, mine_send, mine_recv,
    peer_send, near_recv, peer_recv, inner_send, inner_recv, far_send, far_recv,
    map_send, map_recv, ready,
):
    groups, depth = gathered.shape[0], gathered.shape[1]
    leaves, leaf = diag.shape[0], diag.shape[1]
    rank = u.shape[1]
    block = leaves * rank
    chips = n_rows // 2
    steps = 2 * groups
    last = steps - 1
    c = lax.axis_index("child")
    r = lax.axis_index("rows")
    chip, core = r // 2, r % 2
    partner = chip * 2 + 1 - core

    forward = chips == 4
    if forward:
        x, y = chip % 2, chip // 2
        x_near = (y * 2 + 1 - x) * 2
        y_near = ((1 - y) * 2 + x) * 2
        first = x_near * (1 - core) + y_near * core
        second = y_near * (1 - core) + x_near * core
        across = ((1 - y) * 2 + 1 - x) * 2
        direct = [(second + core, second + core), (first + core, first + core)]
        other = [first + 1 - core, second + 1 - core]
    else:
        direct = [
            (((chip + d) % chips) * 2 + core, ((chip + chips - d) % chips) * 2 + core)
            for d in range(1, chips)
        ]
        other = [((chip + chips - d) % chips) * 2 + 1 - core for d in range(1, chips)]
    sources = [s for _, s in direct]
    if forward:
        sources.append(across + core)
        other.append(across + 1 - core)

    high = c // 2
    beside = c + 1 - 2 * (c % 2)
    peers = [3 - c, (c + 2) % 4, beside]
    is_inner = (c == 1) | (c == 2)
    is_outer = (c == 0) | (c == 3)
    ends = [3 - 3 * high, 2 - high]

    loads = [
        pltpu.make_async_copy(v_hbm.at[0], v, load_sem.at[0]),
        pltpu.make_async_copy(
            omega_hbm.at[0, :, :WIDTH], omega.at[:, :WIDTH], load_sem.at[1]
        ),
        pltpu.make_async_copy(
            omega_hbm.at[0, :, WIDTH:], omega.at[:, WIDTH:], load_sem.at[2]
        ),
        pltpu.make_async_copy(map_hbm, maps, load_sem.at[3]),
        pltpu.make_async_copy(diag_hbm.at[0], diag, load_sem.at[4]),
        pltpu.make_async_copy(coupling_hbm.at[0], coupling, load_sem.at[5]),
        pltpu.make_async_copy(u_hbm.at[0], u, load_sem.at[6]),
    ]
    for load in loads[:2]:
        load.start()

    barrier = pltpu.get_barrier_semaphore()
    for to, _ in direct + [(partner, partner)]:
        pl.semaphore_signal(barrier, inc=1, device_id=(c, to), device_id_type=MESH)
    pl.semaphore_signal(barrier, inc=1, device_id=(beside, r), device_id_type=MESH)

    @pl.when(is_inner)
    def _():
        pl.semaphore_signal(barrier, inc=1, device_id=(3 - c, r), device_id_type=MESH)

    through = (0,)
    summed = steps - len(through)

    def direct_step(s):
        return s in through

    def piece(s, source):
        size = block // 2
        base = (s % 2) * (depth // 2)
        return s // 2, pl.ds(pl.multiple_of(base + source * size, size), size)

    def rows_of(s, source):
        return gathered.at[piece(s, source)]

    def columns(g):
        return slice(g * WIDTH, (g + 1) * WIDTH)

    def project(first, end):
        mask = left_lanes(rank)
        size = block // 2
        values = []
        for i in range(leaves):
            rows = slice(i * leaf, (i + 1) * leaf)
            values.append(
                lax.dot_general(
                    v[rows, :], omega[rows, first * WIDTH : end * WIDTH], (((0,), (0,)), ((), ())),
                    preferred_element_type=jnp.float32,
                )
            )
        for i in range(leaves):
            mine[0, i * rank : (i + 1) * rank, first * WIDTH : end * WIDTH] = values[i].astype(
                jnp.bfloat16
            )
        for i in range(leaves // 2):
            for g in range(first, end):
                cols = columns(g - first)
                low, up = values[i][:, cols], pltpu.roll(values[i + leaves // 2][:, cols], HALF, 1)
                at = pl.multiple_of(r * size + i * rank, rank)
                gathered[g, pl.ds(at, rank), :] = jnp.where(mask, low, up).astype(jnp.bfloat16)
                at = pl.multiple_of(depth // 2 + r * size + i * rank, rank)
                gathered[g, pl.ds(at, rank), :] = jnp.where(mask, up, low).astype(jnp.bfloat16)

    def remote(src, dst, send, recv, to):
        return pltpu.make_async_remote_copy(
            src_ref=src, dst_ref=dst, send_sem=send, recv_sem=recv,
            device_id=to, device_id_type=MESH,
        )

    def ici(t, s):
        at = rows_of(s, r)
        return remote(at, at, ici_send.at[t], ici_recv.at[t, s], (c, direct[t][0]))

    def ici_in(t, s):
        at = rows_of(s, direct[t][1])
        return remote(at, at, ici_send.at[t], ici_recv.at[t, s], (c, direct[t][0]))

    def fwd(s):
        at = rows_of(s, direct[0][1])
        return remote(at, at, fwd_send, fwd_recv.at[s], (c, direct[1][0]))

    def fwd_in(s):
        at = rows_of(s, sources[-1])
        return remote(at, at, fwd_send, fwd_recv.at[s], (c, direct[1][0]))

    def core_kind(t):
        return 1 if forward and t == 2 else 0

    def across_core(t, s, who):
        at = rows_of(s, who[t])
        return remote(at, at, core_send, core_recv.at[core_kind(t), s], (c, partner))

    def to_peer(j, s):
        return remote(
            update.at[s, peers[j]], peer_in.at[s, j],
            peer_send.at[j],
            near_recv.at[s] if j == 2 else peer_recv.at[through.index(s), j],
            (peers[j], r),
        )

    def to_inner(s):
        return remote(
            update.at[s, pl.ds(2 - 2 * high, 2)], inner_in.at[s],
            inner_send, inner_recv.at[s], (beside, r),
        )

    def to_far(e, s):
        return remote(
            sums.at[s, e], far_in.at[s], far_send, far_recv.at[s], (ends[e], r)
        )

    def to_partner():
        return remote(mine.at[0], mine.at[1], mine_send, mine_recv, (c, partner))

    def map_to_peer(j):
        return remote(
            slots.at[peers[j]], slots_in.at[j], map_send.at[0], map_recv.at[0], (peers[j], r)
        )

    def map_to_inner(e):
        return remote(
            slots.at[ends[e]], inner_slots.at[e],
            map_send.at[1], map_recv.at[1], (beside, r),
        )

    def from_partner(s, kind, count):
        at = gathered.at[0, pl.ds(0, count * (block // 2))]
        remote(at, at, core_send, core_recv.at[kind, s], (c, partner)).wait_recv()

    def start(copy):
        copy.start()

    def send_own(t, s):
        if s <= last:
            start(ici(t, s))

    def arrive(t, s):
        if s <= last:
            ici_in(t, s).wait_recv()
            if forward and t == 0:
                start(fwd(s))
            start(across_core(t, s, sources))

    def arrive_across(s):
        fwd_in(s).wait_recv()
        start(across_core(len(sources) - 1, s, sources))

    def part(s, source, fresh=False):
        k = s % 2
        g, at = piece(s, source)
        value = gathered[g, at, :]
        size = block // 2
        for h in range(2):
            cols = pl.ds(pl.multiple_of(source * block + h * size, size), size)
            term = dot(coupling[:, cols], value)
            total[k, h] = term if fresh else total[k, h] + term

    def settle(s):
        k = s % 2
        mask = left_lanes(block)
        known = near_total[:, columns(s // 2)]
        known = jnp.where(mask, known, 0.0) if k == 0 else jnp.where(mask, 0.0, known)
        mixed = jnp.where(mask, total[k, k], total[k, 1 - k]) + known
        coupled[k] = (mixed + pltpu.roll(mixed, HALF, 1)).astype(jnp.bfloat16)

    def local_rows(i):
        value = dot(diag[i], omega[i * leaf : (i + 1) * leaf, :])
        mask = left_lanes(leaf // 2)
        for g in range(groups):
            low = value[: leaf // 2, columns(g)]
            up = pltpu.roll(value[leaf // 2 :, columns(g)], HALF, 1)
            local_part[2 * g, i] = jnp.where(mask, low, up)
            local_part[2 * g + 1, i] = jnp.where(mask, up, low)

    def near_later(s):
        if s >= 0 and not direct_step(s):
            start(to_peer(2, s))

    def finish(s):
        settle(s)
        mask = left_lanes(leaf // 2)
        whole = direct_step(s)
        for e, i in enumerate((peers if whole else ends + [beside]) + [c]):
            rows = pl.ds(pl.multiple_of(i * leaf, leaf), leaf)
            at = pl.ds(pl.multiple_of(i * rank, rank), rank)
            value = dot(u[rows, :], coupled[s % 2, at, :])
            low, up = value[: leaf // 2], value[leaf // 2 :]
            mixed = jnp.where(mask, low, up) if s % 2 == 0 else jnp.where(mask, up, low)
            update[s, i] = (mixed + local_part[s, i]).astype(jnp.bfloat16)
            if whole and e < 3:
                start(to_peer(e, s))
            elif e == 1:
                @pl.when(is_outer)
                def _():
                    to_inner(s).start()
            elif e == 2:
                near_later(s - LATE)

    def spread(value, slot, s):
        value = value.astype(jnp.float32)
        turned = pltpu.roll(value, HALF, 1)
        lanes = lax.broadcasted_iota(jnp.int32, (1, WIDTH), 1)
        main = lanes < HALF if s % 2 == 0 else lanes >= HALF
        s0, s1 = slot[0:1, :], slot[4:5, :]
        held, swapped = jnp.where(main, s0, s1), jnp.where(main, s1, s0)
        want = jnp.where(main, 0.0, 1.0)
        pair = jnp.where(held == want, value, jnp.where(swapped == want, turned, 0.0))
        third = jnp.where(held == 2.0, value, jnp.where(swapped == 2.0, turned, 0.0))
        quarter = leaf // 4
        mask = left_lanes(quarter)
        top, bottom = third[:quarter], third[quarter:]
        folded = jnp.where(mask, top, bottom) if s % 2 == 0 else jnp.where(mask, bottom, top)
        return jnp.concatenate([pair, folded], axis=0)

    def combine(s):
        if s >= 0 and not direct_step(s):
            @pl.when(is_inner)
            def _():
                to_inner(s).wait_recv()
                for e in range(2):
                    value = spread(update[s, ends[e]], slots[ends[e]], s) + spread(
                        inner_in[s, ends[e] - (2 - 2 * high)], inner_slots[e], s
                    )
                    sums[s, e] = value.astype(jnp.bfloat16)
                    to_far(e, s).start()

    def final(s):
        if s < 0:
            return
        value = spread(update[s, c], slots[c], s)
        if direct_step(s):
            for j in reversed(range(3)):
                to_peer(j, s).wait_recv()
                value = value + spread(peer_in[s, j], slots_in[j], s)
        else:
            to_peer(2, s).wait_recv()
            value = value + spread(peer_in[s, 2], slots_in[2], s)
            to_far(0, s).wait_recv()
            value = value + far_in[s].astype(jnp.float32)
        if s % 2 == 0:
            halves[...] = value
        else:
            cols, size, quarter = columns(s // 2), leaf // 2, leaf // 4
            mask = left_lanes(3 * quarter)
            before = halves[...]
            straight = jnp.where(mask, before, value)
            turned = pltpu.roll(jnp.where(mask, value, before), HALF, 1)
            out[0, :, cols] = straight[:size]
            out[1, :, cols] = turned[:size]
            out[2, :quarter, cols] = straight[size:]
            out[2, quarter:, cols] = turned[size:]

    loads[0].wait()
    loads[1].wait()
    for load in loads[2:]:
        load.start()
    project(0, 1)

    @pl.when(is_outer)
    def _():
        pl.semaphore_wait(barrier, len(direct) + 2)

    @pl.when(is_inner)
    def _():
        pl.semaphore_wait(barrier, len(direct) + 3)

    for t in reversed(range(len(direct))):
        send_own(t, 0)
    if forward:
        send_own(0, 1)

    @pl.when(is_inner)
    def _():
        pl.semaphore_signal(ready, inc=1, device_id=(3 - c, r), device_id_type=MESH)

    loads[2].wait()
    project(1, groups)
    to_partner().start()
    for s in range(1, AHEAD):
        send_own(0, s + 1 if forward else s)
        if not forward:
            for t in range(1, len(direct)):
                send_own(t, s)

    def take_maps():
        remote(slots_in, slots_in, map_send.at[0], map_recv.at[0], (beside, r)).wait_recv()

        @pl.when(is_inner)
        def _():
            remote(
                inner_slots, inner_slots, map_send.at[1], map_recv.at[1], (beside, r)
            ).wait_recv()

    def take(s):
        arrive(0, s)
        send_own(1, s + 1)
        send_own(0, s + 1 + AHEAD)

    loads[3].wait()
    for i in range(leaves):
        for b in range(2):
            slot = maps[0, 2 * i + b] - 3 * (r * leaves + i)
            slots[i, 4 * b : 4 * b + 4, :] = jnp.full((4, WIDTH), slot, jnp.int32).astype(
                jnp.float32
            )

    @pl.when(is_inner)
    def _():
        pl.semaphore_wait(ready, 1)
        pl.semaphore_signal(ready, inc=1, device_id=(beside, r), device_id_type=MESH)

    @pl.when(is_outer)
    def _():
        pl.semaphore_wait(ready, 1)

    for j in range(len(peers)):
        map_to_peer(j).start()

    @pl.when(is_outer)
    def _():
        for e in range(2):
            map_to_inner(e).start()

    if forward:
        take(0)
        arrive(1, 0)
        take(1)
    for load in loads[4:]:
        load.wait()
    for i in range(leaves):
        local_rows(i)
    near_total[...] = dot(coupling[:, pl.ds(pl.multiple_of(r * block, block), block)], mine[0])
    to_partner().wait_recv()
    near_total[...] += dot(
        coupling[:, pl.ds(pl.multiple_of(partner * block, block), block)], mine[1]
    )
    if forward:
        part(0, sources[0], True)
        part(0, sources[1])

    for s in range(steps):
        if forward:
            arrive_across(s)
            from_partner(s, 0, 2)
            for source in (other[0], other[1], sources[2]):
                part(s, source)
            if s + 2 <= last:
                take(s + 2)
            if s == 1:
                take_maps()
            combine(s - LAG)
            arrive(1, s + 1)
            if s < last:
                part(s + 1, sources[0], True)
                part(s + 1, sources[1])
            final(s - DONE)
            from_partner(s, 1, 1)
            part(s, other[2])
        else:
            for t in range(len(direct)):
                arrive(t, s)
                send_own(t, s + AHEAD)
            from_partner(s, 0, len(other))
            if s == 1:
                take_maps()
            combine(s - LAG)
            final(s - DONE)

            def more(d, carry, s=s):
                for e in range(2):
                    part(s, (chip + d) % chips * 2 + e)
                return carry

            part(s, (chip + 1) % chips * 2, True)
            part(s, (chip + 1) % chips * 2 + 1)
            lax.fori_loop(2, chips, more, 0)
        finish(s)
    for s in range(last - LATE + 1, steps):
        near_later(s)
    for s in range(last - LAG + 1, last):
        combine(s)
    for s in range(last - DONE + 1, last - 2):
        final(s)
    combine(last)
    for s in range(last - 2, steps):
        final(s)

    def drain(ref, sem):
        remote(ref, ref, sem, map_recv.at[0], (beside, r)).wait_send()

    for t in range(len(direct)):
        drain(gathered.at[:, pl.ds(0, block)], ici_send.at[t])
    if forward:
        drain(gathered.at[:, pl.ds(0, block)], fwd_send)
    drain(gathered.at[:, pl.ds(0, len(sources) * block)], core_send)
    to_partner().wait_send()
    for j in range(2):
        drain(gathered.at[0, pl.ds(0, 128*len(through))], peer_send.at[j])
    drain(update.at[:, 0], peer_send.at[2])
    drain(slots.at[pl.ds(0, len(peers))], map_send.at[0])

    @pl.when(is_outer)
    def _():
        drain(slots.at[pl.ds(0, 2)], map_send.at[1])
        drain(update.at[pl.ds(0, summed), pl.ds(0, 2)], inner_send)

    @pl.when(is_inner)
    def _():
        drain(sums.at[pl.ds(0, summed)], far_send)


def write(value, out, sem):
    copies = [
        pltpu.make_async_copy(value.at[q], out.at[q], sem.at[q]) for q in range(out.shape[0])
    ]
    for copy in copies:
        copy.start()
    for copy in copies:
        copy.wait()


def solution(mesh):
    n_child, n_rows = mesh.shape["child"], mesh.shape["rows"]

    def on_device(omega, leaf_diag, leaf_u, leaf_v, coupling, child_map):
        leaves, leaf = leaf_diag.shape[1], leaf_diag.shape[2]
        rank, samples = leaf_u.shape[2], omega.shape[2]
        groups = samples // WIDTH
        steps = 2 * groups
        block, depth = coupling.shape[1], coupling.shape[2]
        chips = n_rows // 2
        direct = 2 if chips == 4 else chips - 1
        everyone = 1 + direct + (chips == 4)
        peers = n_child - 1
        vmem = pltpu.VMEM
        bf16, f32 = jnp.bfloat16, jnp.float32
        dma = pltpu.SemaphoreType.DMA
        anywhere = pl.BlockSpec(memory_space=pl.ANY)
        shape = (3, leaf // 2, samples)
        value = pl.pallas_call(
            functools.partial(kernel, n_child, n_rows),
            out_shape=vmem(shape, f32),
            in_specs=[anywhere] * 6,
            out_specs=pl.BlockSpec(memory_space=vmem),
            scratch_shapes=[
                vmem((leaves * leaf, samples), bf16),
                vmem((leaves * leaf, rank), bf16),
                vmem((leaves, leaf, leaf), bf16),
                vmem((leaves * leaf, rank), bf16),
                vmem((block, depth), bf16),
                vmem((groups, depth, WIDTH), bf16),
                vmem((2, block, samples), bf16),
                vmem((block, samples), f32),
                vmem((steps, leaves, leaf // 2, WIDTH), f32),
                vmem((2, 2, block, WIDTH), f32),
                vmem((2, block, WIDTH), bf16),
                vmem((steps, leaves, leaf // 2, WIDTH), bf16),
                vmem((steps, 2, 3 * leaf // 4, WIDTH), bf16),
                vmem((steps, peers, leaf // 2, WIDTH), bf16),
                vmem((steps, 2, leaf // 2, WIDTH), bf16),
                vmem((steps, 3 * leaf // 4, WIDTH), bf16),
                vmem((3 * leaf // 4, WIDTH), f32),
                pltpu.SMEM(child_map.shape, jnp.int32),
                vmem((leaves, 8, WIDTH), f32),
                vmem((peers, 8, WIDTH), f32),
                vmem((2, 8, WIDTH), f32),
                dma((7,)),
                dma((direct,)),
                dma((direct, steps)),
                dma,
                dma((steps,)),
                dma,
                dma((2, steps)),
                dma,
                dma,
                dma((peers,)),
                dma((steps,)),
                dma((8, 2)),
                dma,
                dma((steps,)),
                dma,
                dma((steps,)),
                dma((2,)),
                dma((2,)),
                pltpu.SemaphoreType.REGULAR,
            ],
            compiler_params=pltpu.CompilerParams(
                collective_id=0, has_side_effects=True, vmem_limit_bytes=52 * 1024 * 1024
            ),
        )(*[
            pltpu.with_memory_space_constraint(array, pltpu.HBM)
            for array in (omega, leaf_v, child_map, leaf_diag, leaf_u, coupling)
        ])
        value = pltpu.with_memory_space_constraint(value, vmem)
        return pl.pallas_call(
            write,
            out_shape=jax.ShapeDtypeStruct(shape, f32),
            in_specs=[pl.BlockSpec(memory_space=vmem)],
            out_specs=anywhere,
            scratch_shapes=[dma((3,))],
        )(value)

    placed = (
        P("child", "rows", None),
        P("child", "rows", None, None),
        P("child", "rows", None),
        P("child", "rows", None),
        P("child", "rows", None),
        P("child", "rows"),
    )
    return jax.shard_map(
        on_device,
        mesh=mesh,
        in_specs=placed,
        out_specs=P(None, ("child", "rows"), None),
        check_vma=False,
    )
```
